32 devices in a mesh: member: 4 (over z), py: 4 (over x, core), pz: 2 (over y).
Axes of the slice: x: 2, y: 2, z: 4, core: 2. Of those that a mesh axis runs over, the one named last changes fastest.
Arguments:
- velocity_hat: float32 [8, 3, 96, 36864], P('member', None, None, ('py', 'pz')), parts along dimension 0, may hold values from -448 to 448
- time_step: float32 [4], P('member'), parts along dimension 0, may hold values from 0.003 to 0.006
- power: float32 [4], P('member'), parts along dimension 0, may hold values from 20 to 80
- cutoffs: int32 [12], P('member'), parts along dimension 0, may hold values from 48 to 64, as said below
Outputs:
- velocity_next: float32 [8, 3, 96, 36864], P('member', None, None, ('py', 'pz')), parts along dimension 0
- cfl_number: float32 [4], P('member'), parts along dimension 0
- energy: float32 [4], P('member'), parts along dimension 0
The draws below stay inside these ranges and needn't reach their ends.
There are 4 independent parts, one for each index of `member`. The reference program is written for one: setup_inputs(seed, part) draws one part's arguments, and reference() takes and returns one part's arrays. A program takes and returns all parts, laid end to end along the dimension named above; each array names one. Nothing has to cross between parts.
Inputs may be any that keep to these rules, and one draw needn't show every extreme that they name: `cutoffs`: in every draw one of the three equals 64.
All inputs are finite; a program needn't handle non-finite values.
Results may differ from the reference program's by a relative error of at most 0.0002.
Values sent between devices are 32-bit elements; how exact they have to be, the bound alone decides.
A program may use at most 256 MiB of HBM per device.

```python
import math
import jax
import jax.numpy as jnp
from jax import lax

GRID = 192
SECTIONS = 1


def signed_wave(points):
    index = jnp.arange(points, dtype=jnp.int32)
    return jnp.where(index < points // 2, index, index - points)


def draw_velocity_hat(key, part):
    folded = jax.random.fold_in(key, 17)
    noise_key, scale_key = jax.random.split(folded)
    array_shape = (2, 3, GRID // 2, GRID, GRID)
    depth_wave = jnp.arange(GRID // 2, dtype=jnp.int32)[:, None, None]
    across_y = signed_wave(GRID)[None, :, None]
    along_x = signed_wave(GRID)[None, None, :]
    lowest = (depth_wave <= 2) & (jnp.abs(across_y) <= 2) & (jnp.abs(along_x) <= 2)
    values = jnp.clip(jax.random.normal(noise_key, array_shape, jnp.float32), -4.0, 4.0)
    amplify = 64.0
    result = jnp.where(lowest, amplify * values, values).astype(jnp.float32)
    return result.reshape(2, 3, GRID // 2, GRID * GRID)


def draw_cutoffs(key, part):
    folded = jax.random.fold_in(key, 23)
    value_key, pick_key = jax.random.split(folded)
    values = jax.random.randint(value_key, (3,), GRID // 4, GRID // 3 + 1, dtype=jnp.int32)
    chosen = jax.random.randint(pick_key, (), 0, 3, dtype=jnp.int32)
    return jnp.where(jnp.arange(3, dtype=jnp.int32) == chosen, GRID // 3, values).astype(jnp.int32)


def setup_inputs(seed: int = 0, part: int = 0) -> dict:
    key_list = jax.random.split(jax.random.key(seed), 5)
    part_splits = jax.random.split(jax.random.fold_in(key_list[4], part), 5)
    return {
        "velocity_hat": draw_velocity_hat(jax.random.fold_in(jax.random.fold_in(key_list[4], part), 71), part),
        "time_step": jnp.clip(jax.random.uniform(part_splits[1], (1,), jnp.float32, 0.003, 0.006), 0.003, 0.006),
        "power": jnp.clip(jnp.exp(jax.random.uniform(part_splits[2], (1,), jnp.float32, math.log(20.0), math.log(80.0))), 20.0, 80.0),
        "cutoffs": draw_cutoffs(jax.random.fold_in(jax.random.fold_in(key_list[4], part), 71), part),
    }


viscosity = 0.004
keep_share = (0.0, 0.75, 1.0 / 3.0)


def signed_index(points):
    index = jnp.arange(points, dtype=jnp.int32)
    return jnp.where(index < points // 2, index, index - points)


def to_grid(spectra):
    points = spectra.shape[-1]
    result = []
    for component in range(spectra.shape[0]):
        strips = jnp.fft.ifft(jnp.fft.ifft(spectra[component], axis=2), axis=1)
        padded = jnp.concatenate([strips, jnp.zeros_like(strips[:1])], axis=0)
        result.append(jnp.fft.irfft(padded, n=points, axis=0) * (float(points) ** 1.5))
    return jnp.stack(result)


def to_spectrum(fields):
    points = fields.shape[-1]
    result = []
    for component in range(fields.shape[0]):
        planes = jnp.fft.rfft(fields[component], axis=0)[: points // 2]
        result.append(jnp.fft.fft(jnp.fft.fft(planes, axis=1), axis=2) * (float(points) ** -1.5))
    return result


def reference(velocity_hat, time_step, power, cutoffs):
    points = 2 * velocity_hat.shape[2]
    velocity_hat = velocity_hat.reshape(2, 3, points // 2, points, points)
    wave_z = jnp.arange(points // 2, dtype=jnp.int32)[:, None, None]
    wave_y = signed_index(points)[None, :, None]
    wave_x = signed_index(points)[None, None, :]
    keep_mask = ((jnp.abs(wave_x) <= cutoffs[0]) & (jnp.abs(wave_y) <= cutoffs[1]) & (wave_z <= cutoffs[2])).astype(jnp.float32)
    waves = (wave_x.astype(jnp.float32), wave_y.astype(jnp.float32), wave_z.astype(jnp.float32))
    wave_square = waves[0] * waves[0] + waves[1] * waves[1] + waves[2] * waves[2]
    inverse_square = 1.0 / jnp.maximum(wave_square, 1.0)

    def project(field):
        normal_part = waves[0] * field[0] + waves[1] * field[1] + waves[2] * field[2]
        return [keep_mask * (field[axis_index] - waves[axis_index] * normal_part * inverse_square) for axis_index in range(3)]

    step_size = time_step[0]
    current = [lax.complex(velocity_hat[0, axis_index], velocity_hat[1, axis_index]) for axis_index in range(3)]
    initial = current
    cfl_values = []
    energy_values = []
    for section_index in range(SECTIONS):
        solenoidal = project(current)
        if section_index == 0:
            initial = solenoidal
        curled = [waves[1] * solenoidal[2] - waves[2] * solenoidal[1],
                  waves[2] * solenoidal[0] - waves[0] * solenoidal[2],
                  waves[0] * solenoidal[1] - waves[1] * solenoidal[0]]
        vorticity_hat = [1j * term for term in curled]
        physical = to_grid(jnp.stack(solenoidal + vorticity_hat))
        velocity = physical[:3]
        vorticity = physical[3:]
        nonlinear = jnp.stack([velocity[1] * vorticity[2] - velocity[2] * vorticity[1],
                               velocity[2] * vorticity[0] - velocity[0] * vorticity[2],
                               velocity[0] * vorticity[1] - velocity[1] * vorticity[0]])
        fastest = jnp.max(jnp.abs(velocity[0]) + jnp.abs(velocity[1]) + jnp.abs(velocity[2]))
        energy = 0.5 * jnp.sum(velocity * velocity) / float(points ** 3)
        forced = project(to_spectrum(nonlinear))
        forcing = power[0] / jnp.maximum(2.0 * energy, 0.5)
        update = [solenoidal[axis_index] + step_size * (forced[axis_index] + forcing * solenoidal[axis_index] - viscosity * wave_square * solenoidal[axis_index]) for axis_index in range(3)]
        keep_weight = keep_share[section_index]
        current = [keep_weight * initial[axis_index] + (1.0 - keep_weight) * update[axis_index] for axis_index in range(3)]
        cfl_values.append(step_size * fastest * points / (2.0 * math.pi))
        energy_values.append(energy)
    velocity_next = jnp.stack([jnp.stack([jnp.real(term) for term in current]), jnp.stack([jnp.imag(term) for term in current])]).astype(jnp.float32)
    velocity_next = velocity_next.reshape(2, 3, points // 2, points * points)
    return velocity_next, jnp.stack(cfl_values), jnp.stack(energy_values)
```

```python
import functools
import math

import jax
import jax.numpy as jnp
import numpy as np
from jax import lax
from jax.experimental import pallas as pl
from jax.experimental.pallas import tpu as pltpu
from jax.sharding import PartitionSpec as P

viscosity = 0.004
high = lax.Precision.HIGH
TILE = 8
LANES = 128
GROUP = ("py", "pz")
f32 = jnp.float32
bf16 = jnp.bfloat16


def halves(table):
    table = np.asarray(table, np.float32)
    top = table.astype(jnp.bfloat16)
    rest = (table - top.astype(np.float32)).astype(jnp.bfloat16)
    return top, rest


def split(value):
    top = value.astype(bf16)
    return top, (value - top.astype(f32)).astype(bf16)


def signed(index, points):
    return np.where(index < points // 2, index, index - points)


class Sizes:
    def __init__(self, points, group, cross):
        self.points = points
        self.group = group
        self.cross = cross
        self.limit = points // 3
        self.slab = points // group
        self.planes = TILE if self.slab % TILE == 0 else self.slab
        self.chunks = self.slab // self.planes
        self.rows = cross * TILE
        self.window = -(-points // LANES) * LANES
        self.start = (points // LANES) * LANES
        self.pair = 2 * points
        self.above = -(-(self.limit + 1) // cross)
        self.below = -(-self.limit // cross)
        self.scale = float(points) ** -1.5
        assert self.planes <= TILE and 2 * self.limit == LANES and cross % 2 == 0
        assert self.pair % LANES == 0 and self.start + self.window == self.pair

    def pairs_of(self, device):
        mirrored = device >= self.group // 2
        block = self.group - 1 - device if mirrored else device
        kept = self.limit + (0 if mirrored else 1) - block * self.cross
        return -(-min(max(kept, 0), self.cross) // 2)

    def planes_of(self, chunk):
        place = np.arange(TILE)
        plane = np.arange(self.group)[:, None] * self.slab + chunk * self.planes + place
        return np.where(place < self.planes, plane, -1)

    def windows(self, planes):
        lane = np.arange(self.window)
        both = []
        for which, begin in enumerate((0, self.start)):
            index = begin + lane - which * self.points
            wave = signed(index, self.points)
            live = (index >= 0) & (index < self.points) & (np.abs(wave) <= self.limit)
            live = live[None, :] & (planes >= 0)[:, None]
            angle = 2.0 * np.pi * ((planes[:, None] * wave[None, :]) % self.points) / self.points
            both.append((live * np.cos(angle), live * np.sin(angle), live * wave[None, :]))
        return both

    def spread_table(self, chunk):
        tables = []
        for cosine, sine, wave in self.windows(self.planes_of(chunk).reshape(-1)):
            tables.append(np.concatenate([cosine, sine, -wave * sine, wave * cosine]))
        return halves(np.stack(tables))

    def close_table(self):
        planes = np.stack([self.planes_of(c) for c in range(self.chunks)], axis=1).reshape(-1)
        return halves(np.stack([np.concatenate([c, s], axis=1) for c, s, _ in self.windows(planes)]))

    def angle(self, rows, cols):
        return 2.0 * np.pi * (np.outer(rows, cols) % self.points) / self.points

    def cross_tables(self):
        wave = np.arange(1, self.limit + 1)
        angle = self.angle(np.arange(self.points), wave)
        top, rest = halves(np.concatenate([np.cos(angle), np.sin(angle)], axis=1))
        back_top, back_rest = halves(np.concatenate([np.cos(angle), np.sin(angle)], axis=1).T)
        return (np.concatenate([top, top], axis=1), rest, back_top, back_rest)

    def depth_tables(self):
        wave = np.arange(1, self.limit + 1)
        angle = self.angle(wave, np.arange(self.points))
        waves = np.concatenate([np.cos(angle), -np.sin(angle)])
        top, rest = halves(2.0 * self.scale * waves)
        ones = np.ones((LANES, self.points), jnp.bfloat16)
        back_top, back_rest = halves(self.scale * waves.T)
        return (
            np.concatenate([top, top]),
            np.concatenate([rest, ones]),
            np.concatenate([back_top, back_rest], axis=1),
            back_top,
        )


def dot(left, right):
    return jnp.dot(left, right, preferred_element_type=f32)


def dot_rows(left, right):
    return lax.dot_general(left, right, (((1,), (1,)), ((), ())), preferred_element_type=f32)


def turn(value):
    lane = lax.broadcasted_iota(jnp.int32, (1, LANES), 1)
    sign = jnp.where(lane < LANES // 2, -1.0, 1.0).astype(f32)
    return pltpu.roll(value, LANES // 2, 1) * sign


def pair_waves(size, first_cross, cutoffs):
    lane = lax.broadcasted_iota(jnp.int32, (1, size.pair), 1)
    second = (lane >= size.points).astype(jnp.int32)
    along = lane - second * size.points
    along = jnp.where(along < size.points // 2, along, along - size.points)
    cross = first_cross + second
    cross = jnp.where(cross < size.points // 2, cross, cross - size.points)
    depth = lax.broadcasted_iota(jnp.int32, (size.limit, 1), 0) + 1
    keep = (jnp.abs(along) <= cutoffs[0]) & (jnp.abs(cross) <= cutoffs[1])
    keep = keep.astype(f32) * (depth <= cutoffs[2]).astype(f32)
    waves = (along.astype(f32), cross.astype(f32), depth.astype(f32))
    square = waves[0] * waves[0] + waves[1] * waves[1] + waves[2] * waves[2]
    return waves, square, keep


def projected(waves, square, keep, field):
    normal = waves[0] * field[0] + waves[1] * field[1] + waves[2] * field[2]
    normal = normal * (1.0 / jnp.maximum(square, 1.0))
    return [keep * (field[i] - waves[i] * normal) for i in range(3)]


def spread_pair(size, first_cross, mirrored, cutoffs, fields, top_ref, rest_ref, o_ref, base_row):
    waves, square, keep = pair_waves(size, first_cross, cutoffs)
    parts = [projected(waves, square, keep, fields[r]) for r in range(2)]
    whole = [jnp.concatenate([parts[0][i], parts[1][i]], axis=0) for i in range(3)]
    tops, rests = zip(*[split(w) for w in whole])
    count = size.group * TILE
    for which, begin in enumerate((0, size.start)):
        lanes = slice(begin, begin + size.window)
        top, rest = top_ref[which], rest_ref[which]
        x_top, x_rest = tops[0][:, lanes], rests[0][:, lanes]
        ahead = dot_rows(top[: 2 * count], x_top) + dot_rows(top[: 2 * count], x_rest)
        ahead = ahead + dot_rows(rest[: 2 * count], x_top)
        o_top = jnp.concatenate([tops[1][:, lanes], tops[2][:, lanes]], axis=0)
        o_rest = jnp.concatenate([rests[1][:, lanes], rests[2][:, lanes]], axis=0)
        other = dot_rows(top, o_top) + dot_rows(top, o_rest) + dot_rows(rest, o_top)
        results = [ahead[:count] + turn(ahead[count:])]
        for base in (0, 2 * count):
            for i in range(2):
                cols = slice(i * LANES, (i + 1) * LANES)
                results.append(
                    other[base : base + count, cols]
                    + turn(other[base + count : base + 2 * count, cols])
                )
        slot = which + mirrored - 2 * which * mirrored
        at = pl.ds(pl.multiple_of(base_row + slot * TILE, TILE), TILE)
        for g in range(size.group):
            for i in range(5):
                o_ref[g, i, at, :] = results[i][g * TILE : (g + 1) * TILE]


def layer_ahead(size, e_ref, first_row, cross_refs, above, below):
    cross, limit, group = size.cross, size.limit, size.group
    for m in range(size.above):
        above[0, m * cross : (m + 1) * cross, :] = e_ref[m, pl.ds(first_row, cross), :]
    for m in range(size.below):
        below[0, m * cross : (m + 1) * cross, :] = e_ref[group - 1 - m, pl.ds(first_row, cross), :]
    plus, minus = above[0, 1 : limit + 1, :], below[0, :limit, :]
    data = jnp.concatenate([plus + minus, turn(plus - minus)], axis=0)
    top, rest = split(data)
    real = dot(cross_refs[0][...], jnp.concatenate([top, rest], axis=0)) + dot(cross_refs[1][...], top)
    real = (real + above[0, 0:1, :]) * size.scale
    top = real.astype(bf16).astype(f32)
    lane = lax.broadcasted_iota(jnp.int32, (1, LANES), 1)
    return jnp.where(lane < LANES // 2, top, pltpu.roll(real - top, LANES // 2, 1)).astype(bf16)


def layer_back(size, sums, cross_refs):
    limit = size.limit
    top, rest = split(sums)
    waves = dot(cross_refs[2][...], top) + dot(cross_refs[2][...], rest) + dot(cross_refs[3][...], top)
    even, odd = waves[:limit], pltpu.roll(waves[limit:], LANES // 2, 1)
    return even - odd, even + odd, jnp.sum(sums, axis=0, keepdims=True)


def middle_plane(size, plane, r_ref, extra, cross_refs, depth_refs, o_ref, x_ref, s_ref, scratch):
    ya_ref, yb_ref, yc_ref, yd_ref = cross_refs
    za_ref, zb_ref, zc_ref, zd_ref = depth_refs
    above, below, back_above, back_below = scratch
    limit, cross, group, points = size.limit, size.cross, size.group, size.points
    at = pl.ds(plane, cross, stride=TILE)
    sums, turned, firsts = [], [], []
    for i in range(5):
        for m in range(size.above):
            above[i, m * cross : (m + 1) * cross, :] = r_ref[m, i, at, :]
        for m in range(size.below):
            below[i, m * cross : (m + 1) * cross, :] = r_ref[group - 1 - m, i, at, :]
        plus = above[i, 1 : limit + 1, :]
        minus = below[i, :limit, :]
        sums.append(plus + minus)
        turned.append(turn(plus - minus))
        firsts.append(jnp.broadcast_to(above[i, 0:1, :], (TILE, LANES)))
    k = (lax.broadcasted_iota(jnp.int32, (limit, 1), 0) + 1).astype(f32)
    lane = lax.broadcasted_iota(jnp.int32, (1, LANES), 1)
    deep = (lane % limit + 1).astype(f32)
    all_sums = sums[:3] + [
        k * turned[2] - deep * turn(sums[1]),
        deep * turn(sums[0]) - sums[4],
        sums[3] - k * turned[0],
    ]
    all_turned = turned[:3] + [
        -k * sums[2] - deep * turn(turned[1]),
        deep * turn(turned[0]) - turned[4],
        turned[3] + k * sums[0],
    ]
    firsts = firsts[:3] + [
        -deep * turn(firsts[1]),
        deep * turn(firsts[0]) - firsts[4],
        firsts[3],
    ]
    data = jnp.concatenate(
        [jnp.concatenate([all_sums[i], all_turned[i]], axis=0) for i in range(6)], axis=1
    )
    first = jnp.concatenate([f[0:1] for f in firsts], axis=1)
    top, rest = split(data)
    strips = dot(ya_ref[...], jnp.concatenate([top, rest], axis=0)) + dot(yb_ref[...], top) + first
    physical = []
    for i in range(6):
        top, rest = split(strips[:, i * LANES : (i + 1) * LANES])
        mine = ((lane % (LANES // 2)) == i * TILE + plane).astype(f32).astype(bf16)
        physical.append(
            dot(jnp.concatenate([top, rest], axis=1), za_ref[...])
            + dot(jnp.concatenate([top, extra * mine], axis=1), zb_ref[...])
        )
    v, w = physical[:3], physical[3:]
    speed = jnp.abs(v[0]) + jnp.abs(v[1]) + jnp.abs(v[2])
    power = v[0] * v[0] + v[1] * v[1] + v[2] * v[2]
    s_ref[0] = jnp.maximum(s_ref[0], jnp.max(speed.reshape(-1, TILE, points), axis=0))
    s_ref[1] = s_ref[1] + jnp.sum(power.reshape(-1, TILE, points), axis=0)
    nonlinear = [
        v[1] * w[2] - v[2] * w[1],
        v[2] * w[0] - v[0] * w[2],
        v[0] * w[1] - v[1] * w[0],
    ]
    deeps = []
    kept = x_ref[...]
    for i in range(3):
        top, rest = split(nonlinear[i])
        both = dot(top, zc_ref[...])
        deeps.append(both[:, :LANES] + both[:, LANES:] + dot(rest, zd_ref[...]))
        total = jnp.sum(nonlinear[i], axis=1, keepdims=True) * size.scale
        kept = jnp.where(lane == i * TILE + plane, total, kept)
    x_ref[...] = kept
    data = jnp.concatenate(deeps, axis=1)
    top, rest = split(data)
    waves = dot(yc_ref[...], top) + dot(yc_ref[...], rest) + dot(yd_ref[...], top)
    first = jnp.sum(data, axis=0, keepdims=True)
    for i in range(3):
        lanes = slice(i * LANES, (i + 1) * LANES)
        even, odd = waves[:limit, lanes], turn(waves[limit:, lanes])
        back_above[i, 0:1, :] = first[:, lanes]
        back_above[i, 1 : limit + 1, :] = even - odd
        back_below[i, :limit, :] = even + odd
        for m in range(size.above):
            o_ref[m, i, at, :] = back_above[i, m * cross : (m + 1) * cross, :]
        for m in range(size.below):
            o_ref[group - 1 - m, i, at, :] = back_below[i, m * cross : (m + 1) * cross, :]


def section_kernel(size, minor, cut_ref, e_ref, v_ref, top_ref, rest_ref, ya, yb, yc, yd, za, zb, zc, zd,
                   out_ref, last_ref, v_buf, send, recv, e_recv, back, last, sums, stats,
                   above, below, back_above, back_below, v_sem, e_sems, go_sems, come_sems,
                   back_go, back_come, last_go, last_come, own_sems):
    group, cross, chunks, limit = size.group, size.cross, size.chunks, size.limit
    steps = cross // 2
    me = lax.axis_index("py") * minor + lax.axis_index("pz")
    half = group // 2
    mirrored = (me >= half).astype(jnp.int32)
    counts = [size.pairs_of(g) for g in range(group)]
    classes = sorted(set(counts))

    def pairs_at(device):
        block = jnp.where(device >= half, group - 1 - device, device)
        kept = limit + jnp.where(device >= half, 0, 1) - block * cross
        return (jnp.clip(kept, 0, cross) + 1) // 2

    mine = pairs_at(me)
    cutoffs = (cut_ref[0], cut_ref[1], cut_ref[2])
    cross_refs, depth_refs = (ya, yb, yc, yd), (za, zb, zc, zd)
    scratch = (above, below, back_above, back_below)

    def peer(device):
        return {"py": device // minor, "pz": device % minor}

    def peers():
        return [(off, (me + off) % group) for off in range(1, group)]

    def remote(src, dst, go, come, device):
        return pltpu.make_async_remote_copy(
            src_ref=src, dst_ref=dst, send_sem=go, recv_sem=come,
            device_id=peer(device), device_id_type=pl.DeviceIdType.MESH,
        )

    def fetch(p, slot):
        j = p + mirrored * (steps - 1 - 2 * p)
        lanes = pl.ds(pl.multiple_of(j * size.pair, LANES), size.pair)
        return pltpu.make_async_copy(
            v_ref.at[:, :, 0 : v_buf.shape[3], lanes], v_buf.at[slot], v_sem.at[slot]
        )

    @pl.when(mine > 0)
    def _():
        fetch(0, 0).start()

    barrier = pltpu.get_barrier_semaphore()
    for _, device in peers():
        pl.semaphore_signal(barrier, inc=1, device_id=peer(device), device_id_type=pl.DeviceIdType.MESH)
    pl.semaphore_wait(barrier, group - 1)

    def layer_copy(off, device):
        return remote(e_ref.at[device], e_recv.at[me], e_sems.at[0, off], e_sems.at[1, me], device)

    for off, device in peers():
        layer_copy(off, device).start()
    own_layer = pltpu.make_async_copy(e_ref.at[me], e_recv.at[me], own_sems.at[0])
    own_layer.start()

    back_above[...] = jnp.zeros_like(back_above)
    back_below[...] = jnp.zeros_like(back_below)
    back[...] = jnp.zeros_like(back)
    sums[...] = jnp.zeros_like(sums)
    stats[...] = jnp.zeros_like(stats)
    last[...] = jnp.zeros_like(last)

    def spread_step(t, carry):
        chunk, p = t // steps, t % steps

        @pl.when(p < mine)
        def _():
            slot = (chunk * mine + p) % 2
            fetch(p, slot).wait()
            following = jnp.where(p + 1 < mine, p + 1, 0)

            @pl.when((p + 1 < mine) | (chunk + 1 < chunks))
            def _():
                fetch(following, 1 - slot).start()

            j = p + mirrored * (steps - 1 - 2 * p)
            fields = [[v_buf[slot, r, i, 1 : limit + 1, :] for i in range(3)] for r in range(2)]
            spread_pair(
                size, me * cross + 2 * j, mirrored, cutoffs, fields,
                top_ref.at[chunk], rest_ref.at[chunk], send.at[chunk], p * 2 * TILE,
            )
            rows = pl.ds(pl.multiple_of(p * 2 * TILE, 2 * TILE), 2 * TILE)
            for off, device in peers():
                remote(
                    send.at[chunk, device, :, rows, :], recv.at[chunk, me, :, rows, :],
                    go_sems.at[chunk, off], come_sems.at[chunk, me], device,
                ).start()
            pltpu.make_async_copy(
                send.at[chunk, me, :, rows, :], recv.at[chunk, me, :, rows, :], come_sems.at[chunk, me]
            ).start()

        return carry

    lax.fori_loop(0, chunks * steps, spread_step, 0)

    def come_wait(chunk, g):
        ref = recv.at[chunk, g, :, 0 : counts[g] * 2 * TILE, :]
        pltpu.make_async_copy(ref, ref, come_sems.at[chunk, g]).wait()

    def middle_chunk(chunk, carry):
        for g in range(group):
            if counts[g]:
                come_wait(chunk, g)

        @pl.when(chunk == 0)
        def _():
            own_layer.wait()
            for off in range(1, group):
                source = (me + off) % group
                ref = e_recv.at[source]
                pltpu.make_async_copy(ref, ref, e_sems.at[1, source]).wait()

        extra = layer_ahead(size, e_recv, chunk * cross, cross_refs, above, below)

        def plane_step(plane, carry):
            middle_plane(
                size, plane, recv.at[chunk], extra, cross_refs, depth_refs,
                back.at[chunk], sums.at[chunk], stats, scratch,
            )
            return carry

        lax.fori_loop(0, size.planes, plane_step, 0)
        for off, device in peers():
            for n in classes:
                if n:
                    @pl.when(pairs_at(device) == n)
                    def _(n=n, off=off, device=device):
                        rows = slice(0, n * 2 * TILE)
                        remote(
                            back.at[chunk, device, :, rows, :], out_ref.at[chunk, me, :, rows, :],
                            back_go.at[chunk, off], back_come.at[chunk, me], device,
                        ).start()

        for n in classes:
            if n:
                @pl.when(mine == n)
                def _(n=n):
                    rows = slice(0, n * 2 * TILE)
                    pltpu.make_async_copy(
                        back.at[chunk, me, :, rows, :], out_ref.at[chunk, me, :, rows, :],
                        back_come.at[chunk, me],
                    ).start()

        plus, minus, first = layer_back(size, sums[chunk], cross_refs)
        back_above[0, 1 : limit + 1, :] = plus
        back_above[0, 0:1, :] = first
        back_below[0, :limit, :] = minus
        here = pl.ds(chunk * cross, cross)
        for m in range(size.above):
            last[m, here, :] = back_above[0, m * cross : (m + 1) * cross, :]
        for m in range(size.below):
            last[group - 1 - m, here, :] = back_below[0, m * cross : (m + 1) * cross, :]
        return carry

    lax.fori_loop(0, chunks, middle_chunk, 0)
    fastest = jnp.max(stats[0], axis=(0, 1), keepdims=True)
    squares = jnp.sum(stats[1], axis=(0, 1), keepdims=True)
    lane = lax.broadcasted_iota(jnp.int32, (TILE, LANES), 1)
    both = jnp.where(lane == 0, fastest, squares)
    for g in range(group):
        last[g, chunks * cross :, :] = both

    def last_copy(off, device):
        return remote(last.at[device], last_ref.at[me], last_go.at[off], last_come.at[me], device)

    for off, device in peers():
        last_copy(off, device).start()
    own_last = pltpu.make_async_copy(last.at[me], last_ref.at[me], own_sems.at[1])
    own_last.start()

    for off, device in peers():
        layer_copy(off, device).wait_send()
        last_copy(off, device).wait_send()
        ref = last_ref.at[device]
        pltpu.make_async_copy(ref, ref, last_come.at[device]).wait()
    own_last.wait()
    for n in classes:
        if n:
            rows = slice(0, n * 2 * TILE)

            @pl.when(mine == n)
            def _(n=n, rows=rows):
                def sent(chunk, carry):
                    for off in range(1, group):
                        ref = send.at[chunk, off, :, rows, :]
                        pltpu.make_async_copy(ref, ref, go_sems.at[chunk, off]).wait()
                    for g in range(group):
                        ref = out_ref.at[chunk, g, :, rows, :]
                        pltpu.make_async_copy(ref, ref, back_come.at[chunk, g]).wait()
                    return carry

                lax.fori_loop(0, chunks, sent, 0)

    def back_sent(chunk, carry):
        for off, device in peers():
            for n in classes:
                if n:
                    @pl.when(pairs_at(device) == n)
                    def _(n=n, off=off, device=device):
                        ref = back.at[chunk, device, :, 0 : n * 2 * TILE, :]
                        pltpu.make_async_copy(ref, ref, back_go.at[chunk, off]).wait()
        return carry

    lax.fori_loop(0, chunks, back_sent, 0)


def close_kernel(size, place_ref, scalar_ref, v_ref, first_ref, top_ref, rest_ref, *refs):
    r_ref, o_ref = refs
    step = pl.program_id(0)
    limit = size.limit
    results = [[[], []], [[], []], [[], []]]
    for which in range(2):
        slot = jnp.where(place_ref[1] == 1, 1 - which, which)
        at = pl.ds(pl.multiple_of(slot * TILE, TILE), TILE)
        for i in range(3):
            rows = jnp.concatenate(
                [r_ref[c, g, i, at, :] for g in range(size.group) for c in range(size.chunks)], axis=0
            )
            top, rest = split(rows.T)
            out = dot(top, top_ref[which]) + dot(top, rest_ref[which]) + dot(rest, top_ref[which])
            cosine, sine = out[:, : size.window], out[:, size.window :]
            results[i][0].append(cosine[:limit] + sine[limit:])
            results[i][1].append(cosine[limit:] - sine[:limit])

    def joined(low, high_part):
        begin = size.start
        if begin == size.window:
            return jnp.concatenate([low, high_part], axis=1)
        shared = size.window - begin
        return jnp.concatenate(
            [low[:, :begin], low[:, begin:] + high_part[:, :shared], high_part[:, shared:]], axis=1
        )

    waves, square, keep = pair_waves(
        size, place_ref[0] + 2 * step, (place_ref[2], place_ref[3], place_ref[4])
    )
    forcing, step_size = scalar_ref[0], scalar_ref[1]
    gain = 1.0 + step_size * (forcing - viscosity * square)
    depth = o_ref.shape[2]
    for r in range(2):
        solenoidal = projected(
            waves, square, keep, [v_ref[r, i, 1 : limit + 1, :] for i in range(3)]
        )
        forced = projected(waves, square, keep, [joined(*results[i][r]) for i in range(3)])
        for i in range(3):
            o_ref[r, i, 0:1, :] = first_ref[r * 3 + i : r * 3 + i + 1, :]
            o_ref[r, i, 1 : limit + 1, :] = solenoidal[i] * gain + jnp.where(keep > 0.0, step_size * forced[i], 0.0)
            o_ref[r, i, limit + 1 :, :] = jnp.zeros((depth - limit - 1, size.pair), f32)


def whole_block(array):
    return pl.BlockSpec(array.shape, lambda *_: (0,) * array.ndim)


def cost(flops, moved):
    return pl.CostEstimate(flops=int(flops), bytes_accessed=int(moved), transcendentals=0)


def params(megabytes=58):
    return pltpu.CompilerParams(
        dimension_semantics=("arbitrary",), vmem_limit_bytes=megabytes * 1024 * 1024
    )


def section(size, minor, cutoffs, layer, velocity):
    group, chunks, cross, points = size.group, size.chunks, size.cross, size.points
    tops, rests = zip(*[size.spread_table(c) for c in range(chunks)])
    tables = [np.stack(tops), np.stack(rests), *size.cross_tables(), *size.depth_tables()]
    ins = [cutoffs, layer, velocity, *[jnp.asarray(t) for t in tables]]
    kept_rows = -(-(size.limit + 1) // TILE) * TILE
    above = -(-max(size.above * cross, size.limit + 1) // TILE) * TILE
    below = -(-max(size.below * cross, size.limit) // TILE) * TILE
    last_rows = chunks * cross + TILE
    vmem = pl.BlockSpec(memory_space=pltpu.VMEM)
    anywhere = pl.BlockSpec(memory_space=pl.ANY)
    dma = pltpu.SemaphoreType.DMA
    return pl.pallas_call(
        functools.partial(section_kernel, size, minor),
        in_specs=[pl.BlockSpec(memory_space=pltpu.SMEM), vmem, anywhere] + [vmem] * len(tables),
        out_specs=[anywhere, anywhere],
        out_shape=[
            jax.ShapeDtypeStruct((chunks, group, 3, size.rows, LANES), f32),
            jax.ShapeDtypeStruct((group, last_rows, LANES), f32),
        ],
        scratch_shapes=[
            pltpu.VMEM((2, 2, 3, kept_rows, size.pair), f32),
            pltpu.VMEM((chunks, group, 5, size.rows, LANES), f32),
            pltpu.VMEM((chunks, group, 5, size.rows, LANES), f32),
            pltpu.VMEM((group, chunks * cross, LANES), f32),
            pltpu.VMEM((chunks, group, 3, size.rows, LANES), f32),
            pltpu.VMEM((group, last_rows, LANES), f32),
            pltpu.VMEM((chunks, points, LANES), f32),
            pltpu.VMEM((2, TILE, points), f32),
            pltpu.VMEM((5, above, LANES), f32),
            pltpu.VMEM((5, below, LANES), f32),
            pltpu.VMEM((3, above, LANES), f32),
            pltpu.VMEM((3, below, LANES), f32),
            dma((2,)),
            dma((2, group)),
            dma((chunks, group)),
            dma((chunks, group)),
            dma((chunks, group)),
            dma((chunks, group)),
            dma((group,)),
            dma((group,)),
            dma((2,)),
        ],
        compiler_params=pltpu.CompilerParams(
            collective_id=0, has_side_effects=True, vmem_limit_bytes=60 * 1024 * 1024
        ),
        cost_estimate=cost(5e10, 4e7),
        name="section",
    )(*ins)


def close(size, place, scalars, velocity, first, returned):
    top, rest = (jnp.asarray(t) for t in size.close_table())
    steps = size.cross // 2
    block = (2, 3, velocity.shape[2], size.pair)
    return pl.pallas_call(
        functools.partial(close_kernel, size),
        grid_spec=pltpu.PrefetchScalarGridSpec(
            num_scalar_prefetch=1,
            grid=(steps,),
            in_specs=[
                pl.BlockSpec(memory_space=pltpu.SMEM),
                pl.BlockSpec((2, 3, -(-(size.limit + 1) // TILE) * TILE, size.pair), lambda j, p: (0, 0, 0, j)),
                pl.BlockSpec((6, size.pair), lambda j, p: (0, j)),
                whole_block(top),
                whole_block(rest),
                pl.BlockSpec(
                    (size.chunks, size.group, 3, 2 * TILE, LANES),
                    lambda j, p: (0, 0, 0, jnp.where(p[1] == 1, steps - 1 - j, j), 0),
                ),
            ],
            out_specs=pl.BlockSpec(block, lambda j, p: (0, 0, 0, j)),
        ),
        out_shape=jax.ShapeDtypeStruct(velocity.shape, f32),
        compiler_params=params(),
        cost_estimate=cost(5e9, 4e7),
        name="close",
    )(place, scalars, velocity, first, top, rest, returned)


class Shallow:
    def __init__(self, size, velocity, cutoffs, device):
        self.size = size
        points, cross = size.points, size.cross
        layer = velocity[:, :, 0, :].reshape(2, 3, cross, points)
        along = jnp.asarray(signed(np.arange(points), points), jnp.int32)[None, :]
        mirrored = device >= size.group // 2
        spot = lax.broadcasted_iota(jnp.int32, (cross, 1), 0)
        layer = jnp.where(mirrored, layer[:, :, ::-1], layer)
        index = device * cross + jnp.where(mirrored, cross - 1 - spot, spot)
        self.mirrored = mirrored
        across = jnp.where(index < points // 2, index, index - points)
        keep = (jnp.abs(along) <= cutoffs[0]) & (jnp.abs(across) <= cutoffs[1]) & (cutoffs[2] >= 0)
        self.keep = keep.astype(f32)
        self.waves = (along.astype(f32), across.astype(f32), jnp.zeros((1, 1), f32))
        self.square = self.waves[0] ** 2 + self.waves[1] ** 2
        self.layer = jnp.stack(
            [jnp.stack(projected(self.waves, self.square, self.keep, layer[r])) for r in range(2)]
        )
        planes = np.stack([size.planes_of(c) for c in range(size.chunks)], axis=1)
        self.live = (planes >= 0).reshape(-1)
        angle = size.angle(signed(np.arange(points), points), planes.reshape(-1))
        self.cosine = (np.cos(angle) * self.live).astype(np.float32)
        self.sine = (np.sin(angle) * self.live).astype(np.float32)

    def ahead(self):
        size = self.size
        group, chunks, cross = size.group, size.chunks, size.cross

        def turned(x):
            return jnp.stack([-x[1], x[0]])

        u = self.layer
        along, across = self.waves[0], self.waves[1]
        six = jnp.stack(
            [u[:, 0], u[:, 1], u[:, 2], turned(across * u[:, 2]), -turned(along * u[:, 2]),
             turned(along * u[:, 1] - across * u[:, 0])],
            axis=1,
        )
        table = np.concatenate([self.cosine, self.sine], axis=1)
        out = jnp.einsum("rflk,kp->rflp", six, table, precision=high)
        half = self.cosine.shape[1]
        cosine, sine = out[..., :half], out[..., half:]
        grid = jnp.stack([cosine[0] - sine[1], cosine[1] + sine[0]])
        grid = jnp.transpose(grid.reshape(2, 6, cross, group, chunks, TILE), (3, 4, 2, 0, 1, 5))
        grid = grid.reshape(group, chunks * cross, 2, 6 * TILE)
        grid = jnp.pad(grid, ((0, 0), (0, 0), (0, 0), (0, LANES // 2 - 6 * TILE)))
        return grid.reshape(group, chunks * cross, LANES)

    def back(self, got):
        size = self.size
        group, chunks, cross, points = size.group, size.chunks, size.cross, size.points
        numbers = got[:, chunks * cross, :2]
        fastest, squares = jnp.max(numbers[:, 0]), jnp.sum(numbers[:, 1])
        rows = got[:, : chunks * cross].reshape(group, chunks, cross, 2, LANES // 2)
        rows = rows[..., : 3 * TILE].reshape(group, chunks, cross, 2, 3, TILE)
        rows = jnp.transpose(rows, (3, 4, 2, 0, 1, 5)).reshape(2, 3, cross, group * chunks * TILE)
        table = np.concatenate([self.cosine.T, self.sine.T], axis=1)
        out = jnp.einsum("rflp,pk->rflk", rows, table, precision=high)
        cosine, sine = out[..., :points], out[..., points:]
        forced = jnp.stack([cosine[0] + sine[1], cosine[1] - sine[0]])
        forced = jnp.stack(
            [jnp.stack(projected(self.waves, self.square, self.keep, forced[r])) for r in range(2)]
        )
        return forced, fastest, squares


def on_device(velocity, time_step, power, cutoffs):
    group = lax.axis_size("py") * lax.axis_size("pz")
    points = 2 * velocity.shape[2]
    size = Sizes(points, group, velocity.shape[3] // points)
    device = lax.axis_index(GROUP)
    place = jnp.stack(
        [device * size.cross, (device >= group // 2).astype(jnp.int32), cutoffs[0], cutoffs[1], cutoffs[2]]
    ).astype(jnp.int32)
    shallow = Shallow(size, velocity, cutoffs, device)
    returned, got = section(size, lax.axis_size("pz"), cutoffs, shallow.ahead(), velocity)
    forced, fastest, squares = shallow.back(got)
    step_size = time_step[0]
    energy = 0.5 * squares / float(points**3)
    forcing = power[0] / jnp.maximum(2.0 * energy, 0.5)
    gain = 1.0 + step_size * (forcing - viscosity * shallow.square)
    first = shallow.layer * gain + jnp.where(shallow.keep > 0.0, step_size * forced, 0.0)
    first = jnp.where(shallow.mirrored, first[:, :, ::-1], first).reshape(6, size.cross * points)
    velocity_next = close(
        size, place, jnp.stack([forcing, step_size]), velocity, first, returned
    )
    cfl = step_size * fastest * points / (2.0 * math.pi)
    return velocity_next, cfl.reshape(1), energy.reshape(1)


def solution(mesh):
    return jax.shard_map(
        on_device,
        mesh=mesh,
        in_specs=(P("member", None, None, ("py", "pz")), P("member"), P("member"), P("member")),
        out_specs=(P("member", None, None, ("py", "pz")), P("member"), P("member")),
        check_vma=False,
    )
```

```python
import functools
import math

import jax
import jax.numpy as jnp
import numpy as np
from jax import lax
from jax.experimental import pallas as pl
from jax.experimental.pallas import tpu as pltpu
from jax.sharding import PartitionSpec as P

viscosity = 0.004
high = lax.Precision.HIGH
TILE = 8
LANES = 128
GROUP = ("py", "pz")
f32 = jnp.float32
bf16 = jnp.bfloat16


def halves(table):
    table = np.asarray(table, np.float32)
    top = table.astype(jnp.bfloat16)
    rest = (table - top.astype(np.float32)).astype(jnp.bfloat16)
    return top, rest


def split(value):
    top = value.astype(bf16)
    return top, (value - top.astype(f32)).astype(bf16)


def signed(index, points):
    return np.where(index < points // 2, index, index - points)


class Sizes:
    def __init__(self, points, group, cross):
        self.points = points
        self.group = group
        self.cross = cross
        self.limit = points // 3
        self.slab = points // group
        self.planes = TILE if self.slab % TILE == 0 else self.slab
        self.chunks = self.slab // self.planes
        self.rows = cross * TILE
        self.window = -(-points // LANES) * LANES
        self.start = (points // LANES) * LANES
        self.pair = 2 * points
        self.above = -(-(self.limit + 1) // cross)
        self.below = -(-self.limit // cross)
        self.scale = float(points) ** -1.5
        assert self.planes <= TILE and 2 * self.limit == LANES and cross % 2 == 0
        assert self.pair % LANES == 0 and self.start + self.window == self.pair

    def pairs_of(self, device):
        mirrored = device >= self.group // 2
        block = self.group - 1 - device if mirrored else device
        kept = self.limit + (0 if mirrored else 1) - block * self.cross
        return -(-min(max(kept, 0), self.cross) // 2)

    def planes_of(self, chunk):
        place = np.arange(TILE)
        plane = np.arange(self.group)[:, None] * self.slab + chunk * self.planes + place
        return np.where(place < self.planes, plane, -1)

    def windows(self, planes):
        lane = np.arange(self.window)
        both = []
        for which, begin in enumerate((0, self.start)):
            index = begin + lane - which * self.points
            wave = signed(index, self.points)
            live = (index >= 0) & (index < self.points) & (np.abs(wave) <= self.limit)
            live = live[None, :] & (planes >= 0)[:, None]
            angle = 2.0 * np.pi * ((planes[:, None] * wave[None, :]) % self.points) / self.points
            both.append((live * np.cos(angle), live * np.sin(angle)))
        return both

    def spread_table(self, chunk):
        tables = []
        for cosine, sine in self.windows(self.planes_of(chunk).reshape(-1)):
            tables.append(np.concatenate([cosine, sine]))
        return halves(np.stack(tables))

    def close_table(self):
        planes = np.stack([self.planes_of(c) for c in range(self.chunks)], axis=1).reshape(-1)
        return halves(np.stack([np.concatenate([c, s], axis=1) for c, s in self.windows(planes)]))

    def angle(self, rows, cols):
        return 2.0 * np.pi * (np.outer(rows, cols) % self.points) / self.points

    def cross_tables(self):
        wave = np.arange(1, self.limit + 1)
        angle = self.angle(np.arange(self.points), wave)
        top, rest = halves(np.concatenate([np.cos(angle), np.sin(angle)], axis=1))
        back_top, back_rest = halves(np.concatenate([np.cos(angle), np.sin(angle)], axis=1).T)
        return (np.concatenate([top, top], axis=1), rest, back_top, back_rest)

    def depth_tables(self):
        wave = np.arange(1, self.limit + 1)
        angle = self.angle(wave, np.arange(self.points))
        waves = np.concatenate([np.cos(angle), -np.sin(angle)])
        top, rest = halves(2.0 * self.scale * waves)
        ones = np.ones((LANES, self.points), jnp.bfloat16)
        back_top, back_rest = halves(self.scale * waves.T)
        return (
            np.concatenate([top, top]),
            np.concatenate([rest, ones]),
            np.concatenate([back_top, back_rest], axis=1),
            back_top,
        )


def dot(left, right):
    return jnp.dot(left, right, preferred_element_type=f32)


def dot_rows(left, right):
    return lax.dot_general(left, right, (((1,), (1,)), ((), ())), preferred_element_type=f32)


def turn(value):
    lane = lax.broadcasted_iota(jnp.int32, (1, LANES), 1)
    sign = jnp.where(lane < LANES // 2, -1.0, 1.0).astype(f32)
    return pltpu.roll(value, LANES // 2, 1) * sign


def pair_waves(size, first_cross, cutoffs):
    lane = lax.broadcasted_iota(jnp.int32, (1, size.pair), 1)
    second = (lane >= size.points).astype(jnp.int32)
    along = lane - second * size.points
    along = jnp.where(along < size.points // 2, along, along - size.points)
    cross = first_cross + second
    cross = jnp.where(cross < size.points // 2, cross, cross - size.points)
    depth = lax.broadcasted_iota(jnp.int32, (size.limit, 1), 0) + 1
    keep = (jnp.abs(along) <= cutoffs[0]) & (jnp.abs(cross) <= cutoffs[1])
    keep = keep.astype(f32) * (depth <= cutoffs[2]).astype(f32)
    waves = (along.astype(f32), cross.astype(f32), depth.astype(f32))
    square = waves[0] * waves[0] + waves[1] * waves[1] + waves[2] * waves[2]
    return waves, square, keep


def projected(waves, square, keep, field):
    normal = waves[0] * field[0] + waves[1] * field[1] + waves[2] * field[2]
    normal = normal * (1.0 / jnp.maximum(square, 1.0))
    return [keep * (field[i] - waves[i] * normal) for i in range(3)]


def keep_pair(size, first_cross, cutoffs, fields, w_ref):
    waves, square, keep = pair_waves(size, first_cross, cutoffs)
    parts = [projected(waves, square, keep, fields[r]) for r in range(2)]
    whole = [jnp.concatenate([parts[0][i], parts[1][i]], axis=0) for i in range(3)]
    along = waves[0]
    for i in (1, 2):
        whole.append(jnp.concatenate([-along * parts[1][i], along * parts[0][i]], axis=0))
    for i in range(5):
        top, rest = split(whole[i])
        w_ref[0, i] = top
        w_ref[1, i] = rest


def spread_pair(size, mirrored, w_ref, top_ref, rest_ref, o_ref, base_row):
    tops = [w_ref[0, i] for i in range(5)]
    rests = [w_ref[1, i] for i in range(5)]
    count = size.group * TILE
    for which, begin in enumerate((0, size.start)):
        lanes = slice(begin, begin + size.window)
        top, rest = top_ref[which], rest_ref[which]
        results = []
        for fields in ((0,), (1, 2), (3, 4)):
            w_top = jnp.concatenate([tops[i][:, lanes] for i in fields], axis=0)
            w_rest = jnp.concatenate([rests[i][:, lanes] for i in fields], axis=0)
            out = dot_rows(top, w_top) + dot_rows(top, w_rest) + dot_rows(rest, w_top)
            for i in range(len(fields)):
                cols = slice(i * LANES, (i + 1) * LANES)
                results.append(out[:count, cols] + turn(out[count:, cols]))
        slot = which + mirrored - 2 * which * mirrored
        at = pl.ds(pl.multiple_of(base_row + slot * TILE, TILE), TILE)
        for g in range(size.group):
            for i in range(5):
                o_ref[g, i, at, :] = results[i][g * TILE : (g + 1) * TILE]


def layer_ahead(size, e_ref, first_row, cross_refs, above, below):
    cross, limit, group = size.cross, size.limit, size.group
    for m in range(size.above):
        above[0, m * cross : (m + 1) * cross, :] = e_ref[m, pl.ds(first_row, cross), :]
    for m in range(size.below):
        below[0, m * cross : (m + 1) * cross, :] = e_ref[group - 1 - m, pl.ds(first_row, cross), :]
    plus, minus = above[0, 1 : limit + 1, :], below[0, :limit, :]
    data = jnp.concatenate([plus + minus, turn(plus - minus)], axis=0)
    top, rest = split(data)
    real = dot(cross_refs[0][...], jnp.concatenate([top, rest], axis=0)) + dot(cross_refs[1][...], top)
    real = (real + above[0, 0:1, :]) * size.scale
    top = real.astype(bf16).astype(f32)
    lane = lax.broadcasted_iota(jnp.int32, (1, LANES), 1)
    return jnp.where(lane < LANES // 2, top, pltpu.roll(real - top, LANES // 2, 1)).astype(bf16)


def layer_back(size, sums, cross_refs):
    limit = size.limit
    top, rest = split(sums)
    waves = dot(cross_refs[2][...], top) + dot(cross_refs[2][...], rest) + dot(cross_refs[3][...], top)
    even, odd = waves[:limit], pltpu.roll(waves[limit:], LANES // 2, 1)
    return even - odd, even + odd, jnp.sum(sums, axis=0, keepdims=True)


def middle_plane(size, plane, r_ref, extra, cross_refs, depth_refs, o_ref, x_ref, s_ref, scratch):
    ya_ref, yb_ref, yc_ref, yd_ref = cross_refs
    za_ref, zb_ref, zc_ref, zd_ref = depth_refs
    above, below, back_above, back_below = scratch
    limit, cross, group, points = size.limit, size.cross, size.group, size.points
    at = pl.ds(plane, cross, stride=TILE)
    sums, turned, firsts = [], [], []
    for i in range(5):
        for m in range(size.above):
            above[i, m * cross : (m + 1) * cross, :] = r_ref[m, i, at, :]
        for m in range(size.below):
            below[i, m * cross : (m + 1) * cross, :] = r_ref[group - 1 - m, i, at, :]
        plus = above[i, 1 : limit + 1, :]
        minus = below[i, :limit, :]
        sums.append(plus + minus)
        turned.append(turn(plus - minus))
        firsts.append(jnp.broadcast_to(above[i, 0:1, :], (TILE, LANES)))
    k = (lax.broadcasted_iota(jnp.int32, (limit, 1), 0) + 1).astype(f32)
    lane = lax.broadcasted_iota(jnp.int32, (1, LANES), 1)
    deep = (lane % limit + 1).astype(f32)
    all_sums = sums[:3] + [
        k * turned[2] - deep * turn(sums[1]),
        deep * turn(sums[0]) - sums[4],
        sums[3] - k * turned[0],
    ]
    all_turned = turned[:3] + [
        -k * sums[2] - deep * turn(turned[1]),
        deep * turn(turned[0]) - turned[4],
        turned[3] + k * sums[0],
    ]
    firsts = firsts[:3] + [
        -deep * turn(firsts[1]),
        deep * turn(firsts[0]) - firsts[4],
        firsts[3],
    ]
    data = jnp.concatenate(
        [jnp.concatenate([all_sums[i], all_turned[i]], axis=0) for i in range(6)], axis=1
    )
    first = jnp.concatenate([f[0:1] for f in firsts], axis=1)
    top, rest = split(data)
    strips = dot(ya_ref[...], jnp.concatenate([top, rest], axis=0)) + dot(yb_ref[...], top) + first
    physical = []
    for i in range(6):
        top, rest = split(strips[:, i * LANES : (i + 1) * LANES])
        mine = ((lane % (LANES // 2)) == i * TILE + plane).astype(f32).astype(bf16)
        physical.append(
            dot(jnp.concatenate([top, rest], axis=1), za_ref[...])
            + dot(jnp.concatenate([top, extra * mine], axis=1), zb_ref[...])
        )
    v, w = physical[:3], physical[3:]
    speed = jnp.abs(v[0]) + jnp.abs(v[1]) + jnp.abs(v[2])
    power = v[0] * v[0] + v[1] * v[1] + v[2] * v[2]
    s_ref[0] = jnp.maximum(s_ref[0], jnp.max(speed.reshape(-1, TILE, points), axis=0))
    s_ref[1] = s_ref[1] + jnp.sum(power.reshape(-1, TILE, points), axis=0)
    nonlinear = [
        v[1] * w[2] - v[2] * w[1],
        v[2] * w[0] - v[0] * w[2],
        v[0] * w[1] - v[1] * w[0],
    ]
    deeps = []
    kept = x_ref[...]
    for i in range(3):
        top, rest = split(nonlinear[i])
        both = dot(top, zc_ref[...])
        deeps.append(both[:, :LANES] + both[:, LANES:] + dot(rest, zd_ref[...]))
        total = jnp.sum(nonlinear[i], axis=1, keepdims=True) * size.scale
        kept = jnp.where(lane == i * TILE + plane, total, kept)
    x_ref[...] = kept
    data = jnp.concatenate(deeps, axis=1)
    top, rest = split(data)
    waves = dot(yc_ref[...], top) + dot(yc_ref[...], rest) + dot(yd_ref[...], top)
    first = jnp.sum(data, axis=0, keepdims=True)
    for i in range(3):
        lanes = slice(i * LANES, (i + 1) * LANES)
        even, odd = waves[:limit, lanes], turn(waves[limit:, lanes])
        back_above[i, 0:1, :] = first[:, lanes]
        back_above[i, 1 : limit + 1, :] = even - odd
        back_below[i, :limit, :] = even + odd
        for m in range(size.above):
            o_ref[m, i, at, :] = back_above[i, m * cross : (m + 1) * cross, :]
        for m in range(size.below):
            o_ref[group - 1 - m, i, at, :] = back_below[i, m * cross : (m + 1) * cross, :]


def section_kernel(size, minor, cut_ref, e_ref, v_ref, top_ref, rest_ref, ya, yb, yc, yd, za, zb, zc, zd,
                   out_ref, last_ref, place_ref, v_buf, send, recv, e_recv, back, last, sums, stats,
                   above, below, back_above, back_below, v_sem, e_sems, go_sems, come_sems,
                   back_go, back_come, last_go, last_come, own_sems, halves_buf):
    group, cross, chunks, limit = size.group, size.cross, size.chunks, size.limit
    steps = cross // 2
    me = lax.axis_index("py") * minor + lax.axis_index("pz")
    half = group // 2
    mirrored = (me >= half).astype(jnp.int32)
    counts = [size.pairs_of(g) for g in range(group)]
    classes = sorted(set(counts))

    def pairs_at(device):
        block = jnp.where(device >= half, group - 1 - device, device)
        kept = limit + jnp.where(device >= half, 0, 1) - block * cross
        return (jnp.clip(kept, 0, cross) + 1) // 2

    mine = pairs_at(me)
    place_ref[0] = me * cross
    place_ref[1] = mirrored
    for i in range(3):
        place_ref[2 + i] = cut_ref[i]
    cutoffs = (cut_ref[0], cut_ref[1], cut_ref[2])
    cross_refs, depth_refs = (ya, yb, yc, yd), (za, zb, zc, zd)
    scratch = (above, below, back_above, back_below)

    def peer(device):
        return {"py": device // minor, "pz": device % minor}

    def peers():
        return [(off, (me + off) % group) for off in range(1, group)]

    def remote(src, dst, go, come, device):
        return pltpu.make_async_remote_copy(
            src_ref=src, dst_ref=dst, send_sem=go, recv_sem=come,
            device_id=peer(device), device_id_type=pl.DeviceIdType.MESH,
        )

    def fetch(p, slot):
        j = p + mirrored * (steps - 1 - 2 * p)
        lanes = pl.ds(pl.multiple_of(j * size.pair, LANES), size.pair)
        return pltpu.make_async_copy(
            v_ref.at[:, :, 0 : v_buf.shape[3], lanes], v_buf.at[slot], v_sem.at[slot]
        )

    @pl.when(mine > 0)
    def _():
        fetch(0, 0).start()

    barrier = pltpu.get_barrier_semaphore()
    for _, device in peers():
        pl.semaphore_signal(barrier, inc=1, device_id=peer(device), device_id_type=pl.DeviceIdType.MESH)
    pl.semaphore_wait(barrier, group - 1)

    def layer_copy(off, device):
        return remote(e_ref.at[device], e_recv.at[me], e_sems.at[0, off], e_sems.at[1, me], device)

    for off, device in peers():
        layer_copy(off, device).start()
    own_layer = pltpu.make_async_copy(e_ref.at[me], e_recv.at[me], own_sems.at[0])
    own_layer.start()

    back_above[...] = jnp.zeros_like(back_above)
    back_below[...] = jnp.zeros_like(back_below)
    back[...] = jnp.zeros_like(back)
    sums[...] = jnp.zeros_like(sums)
    stats[...] = jnp.zeros_like(stats)
    last[...] = jnp.zeros_like(last)

    def spread_step(t, carry):
        chunk, p = t // steps, t % steps

        @pl.when(p < mine)
        def _():
            @pl.when(chunk == 0)
            def _():
                slot = p % 2
                fetch(p, slot).wait()

                @pl.when(p + 1 < mine)
                def _():
                    fetch(p + 1, 1 - slot).start()

                j = p + mirrored * (steps - 1 - 2 * p)
                fields = [[v_buf[slot, r, i, 1 : limit + 1, :] for i in range(3)] for r in range(2)]
                keep_pair(size, me * cross + 2 * j, cutoffs, fields, halves_buf.at[p])

            spread_pair(
                size, mirrored, halves_buf.at[p],
                top_ref.at[chunk], rest_ref.at[chunk], send.at[chunk], p * 2 * TILE,
            )
            rows = pl.ds(pl.multiple_of(p * 2 * TILE, 2 * TILE), 2 * TILE)
            for off, device in peers():
                remote(
                    send.at[chunk, device, :, rows, :], recv.at[chunk, me, :, rows, :],
                    go_sems.at[chunk, off], come_sems.at[chunk, me], device,
                ).start()
            recv[chunk, me, :, rows, :] = send[chunk, me, :, rows, :]

        return carry

    lax.fori_loop(0, chunks * steps, spread_step, 0)

    def come_wait(chunk, g):
        ref = recv.at[chunk, g, :, 0 : counts[g] * 2 * TILE, :]
        pltpu.make_async_copy(ref, ref, come_sems.at[chunk, g]).wait()

    def middle_chunk(chunk, carry):
        for g in range(group):
            if counts[g]:
                pl.when(me != g)(lambda g=g: come_wait(chunk, g))

        @pl.when(chunk == 0)
        def _():
            own_layer.wait()
            for off in range(1, group):
                source = (me + off) % group
                ref = e_recv.at[source]
                pltpu.make_async_copy(ref, ref, e_sems.at[1, source]).wait()

        extra = layer_ahead(size, e_recv, chunk * cross, cross_refs, above, below)

        def plane_step(plane, carry):
            middle_plane(
                size, plane, recv.at[chunk], extra, cross_refs, depth_refs,
                back.at[chunk], sums.at[chunk], stats, scratch,
            )
            return carry

        lax.fori_loop(0, size.planes, plane_step, 0)
        for off, device in peers():
            for n in classes:
                if n:
                    @pl.when(pairs_at(device) == n)
                    def _(n=n, off=off, device=device):
                        rows = slice(0, n * 2 * TILE)
                        remote(
                            back.at[chunk, device, :, rows, :], out_ref.at[chunk, me, :, rows, :],
                            back_go.at[chunk, off], back_come.at[chunk, me], device,
                        ).start()

        for n in classes:
            if n:
                @pl.when(mine == n)
                def _(n=n):
                    rows = slice(0, n * 2 * TILE)
                    pltpu.make_async_copy(
                        back.at[chunk, me, :, rows, :], out_ref.at[chunk, me, :, rows, :],
                        back_come.at[chunk, me],
                    ).start()

        plus, minus, first = layer_back(size, sums[chunk], cross_refs)
        back_above[0, 1 : limit + 1, :] = plus
        back_above[0, 0:1, :] = first
        back_below[0, :limit, :] = minus
        here = pl.ds(chunk * cross, cross)
        for m in range(size.above):
            last[m, here, :] = back_above[0, m * cross : (m + 1) * cross, :]
        for m in range(size.below):
            last[group - 1 - m, here, :] = back_below[0, m * cross : (m + 1) * cross, :]
        return carry

    lax.fori_loop(0, chunks, middle_chunk, 0)
    fastest = jnp.max(stats[0], axis=(0, 1), keepdims=True)
    squares = jnp.sum(stats[1], axis=(0, 1), keepdims=True)
    lane = lax.broadcasted_iota(jnp.int32, (TILE, LANES), 1)
    both = jnp.where(lane == 0, fastest, squares)
    for g in range(group):
        last[g, chunks * cross :, :] = both

    def last_copy(off, device):
        return remote(last.at[device], last_ref.at[me], last_go.at[off], last_come.at[me], device)

    for off, device in peers():
        last_copy(off, device).start()
    own_last = pltpu.make_async_copy(last.at[me], last_ref.at[me], own_sems.at[1])
    own_last.start()

    for off, device in peers():
        layer_copy(off, device).wait_send()
        last_copy(off, device).wait_send()
        ref = last_ref.at[device]
        pltpu.make_async_copy(ref, ref, last_come.at[device]).wait()
    own_last.wait()
    for n in classes:
        if n:
            rows = slice(0, n * 2 * TILE)

            @pl.when(mine == n)
            def _(n=n, rows=rows):
                def sent(chunk, carry):
                    for off in range(1, group):
                        ref = send.at[chunk, off, :, rows, :]
                        pltpu.make_async_copy(ref, ref, go_sems.at[chunk, off]).wait()
                    for g in range(group):
                        ref = out_ref.at[chunk, g, :, rows, :]
                        pltpu.make_async_copy(ref, ref, back_come.at[chunk, g]).wait()
                    return carry

                lax.fori_loop(0, chunks, sent, 0)

    def back_sent(chunk, carry):
        for off, device in peers():
            for n in classes:
                if n:
                    @pl.when(pairs_at(device) == n)
                    def _(n=n, off=off, device=device):
                        ref = back.at[chunk, device, :, 0 : n * 2 * TILE, :]
                        pltpu.make_async_copy(ref, ref, back_go.at[chunk, off]).wait()
        return carry

    lax.fori_loop(0, chunks, back_sent, 0)


def close_kernel(size, place_ref, scalar_ref, first_ref, top_ref, rest_ref, *refs):
    v_refs, refs = refs[:6], refs[6:]
    r_refs, (out_ref, o_buf, o_sem) = refs[: size.chunks], refs[size.chunks :]
    step, steps = pl.program_id(0), pl.num_programs(0)
    buffer = step % 2
    o_ref = o_buf.at[buffer]

    def leave(at, slot):
        lanes = pl.ds(pl.multiple_of(at * size.pair, LANES), size.pair)
        return [
            pltpu.make_async_copy(
                o_buf.at[slot, r, i], out_ref.at[r, i, :, lanes], o_sem.at[slot, 3 * r + i]
            )
            for r in range(2)
            for i in range(3)
        ]

    @pl.when(step < 2)
    def _():
        o_ref[:, :, size.limit + 1 :, :] = jnp.zeros(
            (2, 3, o_buf.shape[3] - size.limit - 1, size.pair), f32
        )

    @pl.when(step >= 2)
    def _():
        for copy in leave(step - 2, buffer):
            copy.wait()

    limit = size.limit
    results = [[[], []], [[], []], [[], []]]
    for which in range(2):
        slot = jnp.where(place_ref[1] == 1, 1 - which, which)
        at = pl.ds(pl.multiple_of(slot * TILE, TILE), TILE)
        for i in range(3):
            rows = jnp.concatenate(
                [r[0, g, i, at, :] for g in range(size.group) for r in r_refs], axis=0
            )
            top, rest = split(rows.T)
            out = dot(top, top_ref[which]) + dot(top, rest_ref[which]) + dot(rest, top_ref[which])
            cosine, sine = out[:, : size.window], out[:, size.window :]
            results[i][0].append(cosine[:limit] + sine[limit:])
            results[i][1].append(cosine[limit:] - sine[:limit])

    def joined(low, high_part):
        begin = size.start
        if begin == size.window:
            return jnp.concatenate([low, high_part], axis=1)
        shared = size.window - begin
        return jnp.concatenate(
            [low[:, :begin], low[:, begin:] + high_part[:, :shared], high_part[:, shared:]], axis=1
        )

    waves, square, keep = pair_waves(
        size, place_ref[0] + 2 * step, (place_ref[2], place_ref[3], place_ref[4])
    )
    forcing, step_size = scalar_ref[0], scalar_ref[1]
    gain = 1.0 + step_size * (forcing - viscosity * square)
    for r in range(2):
        solenoidal = projected(
            waves, square, keep, [v_refs[3 * r + i][0, 0, 1 : limit + 1, :] for i in range(3)]
        )
        forced = projected(waves, square, keep, [joined(*results[i][r]) for i in range(3)])
        for i in range(3):
            o_ref[r, i, 0:1, :] = first_ref[r * 3 + i : r * 3 + i + 1, :]
            o_ref[r, i, 1 : limit + 1, :] = solenoidal[i] * gain + jnp.where(keep > 0.0, step_size * forced[i], 0.0)


    for copy in leave(step, buffer):
        copy.start()

    @pl.when(step == steps - 1)
    def _():
        for copy in leave(step - 1, 1 - buffer) + leave(step, buffer):
            copy.wait()


def whole_block(array):
    return pl.BlockSpec(array.shape, lambda *_: (0,) * array.ndim)


def cost(flops, moved):
    return pl.CostEstimate(flops=int(flops), bytes_accessed=int(moved), transcendentals=0)


def params(megabytes=58):
    return pltpu.CompilerParams(
        dimension_semantics=("arbitrary",), vmem_limit_bytes=megabytes * 1024 * 1024
    )


def section(size, minor, cutoffs, layer, velocity):
    group, chunks, cross, points = size.group, size.chunks, size.cross, size.points
    tops, rests = zip(*[size.spread_table(c) for c in range(chunks)])
    tables = [np.stack(tops), np.stack(rests), *size.cross_tables(), *size.depth_tables()]
    ins = [cutoffs, layer, velocity, *[jnp.asarray(t) for t in tables]]
    kept_rows = -(-(size.limit + 1) // TILE) * TILE
    above = -(-max(size.above * cross, size.limit + 1) // TILE) * TILE
    below = -(-max(size.below * cross, size.limit) // TILE) * TILE
    last_rows = chunks * cross + TILE
    vmem = pl.BlockSpec(memory_space=pltpu.VMEM)
    anywhere = pl.BlockSpec(memory_space=pl.ANY)
    dma = pltpu.SemaphoreType.DMA
    return pl.pallas_call(
        functools.partial(section_kernel, size, minor),
        in_specs=[pl.BlockSpec(memory_space=pltpu.SMEM), vmem, anywhere] + [vmem] * len(tables),
        out_specs=[anywhere, anywhere, pl.BlockSpec(memory_space=pltpu.SMEM)],
        out_shape=[
            jax.ShapeDtypeStruct((chunks, group, 3, size.rows, LANES), f32),
            jax.ShapeDtypeStruct((group, last_rows, LANES), f32),
            jax.ShapeDtypeStruct((5,), jnp.int32),
        ],
        scratch_shapes=[
            pltpu.VMEM((2, 2, 3, kept_rows, size.pair), f32),
            pltpu.VMEM((chunks, group, 5, size.rows, LANES), f32),
            pltpu.VMEM((chunks, group, 5, size.rows, LANES), f32),
            pltpu.VMEM((group, chunks * cross, LANES), f32),
            pltpu.VMEM((chunks, group, 3, size.rows, LANES), f32),
            pltpu.VMEM((group, last_rows, LANES), f32),
            pltpu.VMEM((chunks, points, LANES), f32),
            pltpu.VMEM((2, TILE, points), f32),
            pltpu.VMEM((5, above, LANES), f32),
            pltpu.VMEM((5, below, LANES), f32),
            pltpu.VMEM((3, above, LANES), f32),
            pltpu.VMEM((3, below, LANES), f32),
            dma((2,)),
            dma((2, group)),
            dma((chunks, group)),
            dma((chunks, group)),
            dma((chunks, group)),
            dma((chunks, group)),
            dma((group,)),
            dma((group,)),
            dma((2,)),
            pltpu.VMEM((cross // 2, 2, 5, LANES, size.pair), bf16),
        ],
        compiler_params=pltpu.CompilerParams(
            collective_id=0, has_side_effects=True, vmem_limit_bytes=60 * 1024 * 1024
        ),
        cost_estimate=cost(5e10, 4e7),
        name="section",
    )(*ins)


def close(size, place, scalars, velocity, first, returned):
    top, rest = (jnp.asarray(t) for t in size.close_table())
    steps = size.cross // 2
    kept_rows = -(-(size.limit + 1) // TILE) * TILE

    def part(r, i):
        return pl.BlockSpec((1, 1, kept_rows, size.pair), lambda j, p: (r, i, 0, j))

    def chunk_block(c):
        return pl.BlockSpec(
            (1, size.group, 3, 2 * TILE, LANES),
            lambda j, p: (c, 0, 0, jnp.where(p[1] == 1, steps - 1 - j, j), 0),
        )

    return pl.pallas_call(
        functools.partial(close_kernel, size),
        grid_spec=pltpu.PrefetchScalarGridSpec(
            num_scalar_prefetch=1,
            grid=(steps,),
            in_specs=[
                pl.BlockSpec(memory_space=pltpu.SMEM),
                pl.BlockSpec((6, size.pair), lambda j, p: (0, j)),
                whole_block(top),
                whole_block(rest),
                *[part(r, i) for r in range(2) for i in range(3)],
                *[chunk_block(c) for c in range(size.chunks)],
            ],
            out_specs=pl.BlockSpec(memory_space=pl.ANY),
            scratch_shapes=[
                pltpu.VMEM((2, 2, 3, velocity.shape[2], size.pair), f32),
                pltpu.SemaphoreType.DMA((2, 6)),
            ],
        ),
        out_shape=jax.ShapeDtypeStruct(velocity.shape, f32),
        compiler_params=params(),
        cost_estimate=cost(5e9, 4e7),
        name="close",
    )(place, scalars, first, top, rest, *[velocity] * 6, *[returned] * size.chunks)


class Shallow:
    def __init__(self, size, velocity, cutoffs, device):
        self.size = size
        points, cross = size.points, size.cross
        layer = velocity[:, :, 0, :].reshape(2, 3, cross, points)
        along = jnp.asarray(signed(np.arange(points), points), jnp.int32)[None, :]
        mirrored = device >= size.group // 2
        spot = lax.broadcasted_iota(jnp.int32, (cross, 1), 0)
        layer = jnp.where(mirrored, layer[:, :, ::-1], layer)
        index = device * cross + jnp.where(mirrored, cross - 1 - spot, spot)
        self.mirrored = mirrored
        across = jnp.where(index < points // 2, index, index - points)
        bounds = cutoffs.reshape(3, 1)
        keep = (jnp.abs(along) <= bounds[0:1]) & (jnp.abs(across) <= bounds[1:2]) & (bounds[2:3] >= 0)
        self.keep = keep.astype(f32)
        self.waves = (along.astype(f32), across.astype(f32), jnp.zeros((1, 1), f32))
        self.square = self.waves[0] ** 2 + self.waves[1] ** 2
        self.layer = jnp.stack(
            [jnp.stack(projected(self.waves, self.square, self.keep, layer[r])) for r in range(2)]
        )
        planes = np.stack([size.planes_of(c) for c in range(size.chunks)], axis=1)
        self.live = (planes >= 0).reshape(-1)
        angle = size.angle(signed(np.arange(points), points), planes.reshape(-1))
        self.cosine = (np.cos(angle) * self.live).astype(np.float32)
        self.sine = (np.sin(angle) * self.live).astype(np.float32)

    def ahead(self):
        size = self.size
        group, chunks, cross = size.group, size.chunks, size.cross

        def turned(x):
            return jnp.stack([-x[1], x[0]])

        u = self.layer
        along, across = self.waves[0], self.waves[1]
        six = jnp.stack(
            [u[:, 0], u[:, 1], u[:, 2], turned(across * u[:, 2]), -turned(along * u[:, 2]),
             turned(along * u[:, 1] - across * u[:, 0])],
            axis=1,
        )
        table = np.concatenate([self.cosine, self.sine], axis=1)
        out = jnp.einsum("rflk,kp->rflp", six, table, precision=high)
        half = self.cosine.shape[1]
        cosine, sine = out[..., :half], out[..., half:]
        grid = jnp.stack([cosine[0] - sine[1], cosine[1] + sine[0]])
        grid = jnp.transpose(grid.reshape(2, 6, cross, group, chunks, TILE), (3, 4, 2, 0, 1, 5))
        grid = grid.reshape(group, chunks * cross, 2, 6 * TILE)
        grid = jnp.pad(grid, ((0, 0), (0, 0), (0, 0), (0, LANES // 2 - 6 * TILE)))
        return grid.reshape(group, chunks * cross, LANES)

    def back(self, got):
        size = self.size
        group, chunks, cross, points = size.group, size.chunks, size.cross, size.points
        numbers = got[:, chunks * cross, :2]
        fastest, squares = jnp.max(numbers[:, 0]), jnp.sum(numbers[:, 1])
        rows = got[:, : chunks * cross].reshape(group, chunks, cross, 2, LANES // 2)
        rows = rows[..., : 3 * TILE].reshape(group, chunks, cross, 2, 3, TILE)
        rows = jnp.transpose(rows, (3, 4, 2, 0, 1, 5)).reshape(2, 3, cross, group * chunks * TILE)
        table = np.concatenate([self.cosine.T, self.sine.T], axis=1)
        out = jnp.einsum("rflp,pk->rflk", rows, table, precision=high)
        cosine, sine = out[..., :points], out[..., points:]
        forced = jnp.stack([cosine[0] + sine[1], cosine[1] - sine[0]])
        forced = jnp.stack(
            [jnp.stack(projected(self.waves, self.square, self.keep, forced[r])) for r in range(2)]
        )
        return forced, fastest, squares


def on_device(velocity, time_step, power, cutoffs):
    group = lax.axis_size("py") * lax.axis_size("pz")
    points = 2 * velocity.shape[2]
    size = Sizes(points, group, velocity.shape[3] // points)
    device = lax.axis_index(GROUP)
    shallow = Shallow(size, velocity, cutoffs, device)
    returned, got, place = section(size, lax.axis_size("pz"), cutoffs, shallow.ahead(), velocity)
    forced, fastest, squares = shallow.back(got)
    step_size = time_step[0]
    energy = 0.5 * squares / float(points**3)
    forcing = power[0] / jnp.maximum(2.0 * energy, 0.5)
    gain = 1.0 + step_size * (forcing - viscosity * shallow.square)
    first = shallow.layer * gain + jnp.where(shallow.keep > 0.0, step_size * forced, 0.0)
    first = jnp.where(shallow.mirrored, first[:, :, ::-1], first).reshape(6, size.cross * points)
    velocity_next = close(
        size, place, jnp.stack([forcing, step_size]), velocity, first, returned
    )
    cfl = step_size * fastest * points / (2.0 * math.pi)
    return velocity_next, cfl.reshape(1), energy.reshape(1)


def solution(mesh):
    return jax.shard_map(
        on_device,
        mesh=mesh,
        in_specs=(P("member", None, None, ("py", "pz")), P("member"), P("member"), P("member")),
        out_specs=(P("member", None, None, ("py", "pz")), P("member"), P("member")),
        check_vma=False,
    )
```
